32 devices in a mesh: grp: 4 (over z), row: 8 (over y, x, core).
Axes of the slice: x: 2, y: 2, z: 4, core: 2. Of those that a mesh axis runs over, the one named last changes fastest.
Arguments:
- expert_grams: float32 [4, 4096, 4096], P(None, 'row'), may hold values from -32 to 48, as said below
- expert_weights: bfloat16 [4, 4096, 512], P(None, 'row', 'grp'), may hold values from -6 to 6
Outputs:
- merged: float32 [4096, 512], P('row', 'grp')
- residual_ratio: float32 [], replicated
The draws below stay inside these ranges and needn't reach their ends.
Inputs may be any that keep to these rules, and one draw needn't show every extreme that they name: Each expert_grams[k] is exactly symmetric and positive definite.
All inputs are finite; a program needn't handle non-finite values.
Results may differ from the reference program's by a relative error of at most 0.0003.
Values may be sent and summed in bfloat16 or wider, within the bound.
A program may use at most 128 MiB of HBM per device.

```python
import jax
import jax.numpy as jnp
from jax import lax

D = 4096
EXPERTS = 4
ITERS = 4
COLS = 512


def one_gram(key, expert_index):
    expert_key = jax.random.fold_in(key, 7919 + expert_index)
    sample_key, diagonal_key, common_key = jax.random.split(expert_key, 3)
    samples = D // 8
    samples_matrix = jnp.clip(jax.random.normal(sample_key, (samples, D), jnp.float32), -4.0, 4.0)
    diagonal = jnp.exp(jax.random.uniform(diagonal_key, (D,), jnp.float32, jnp.log(0.05), 0.0))
    raw_gram = jnp.dot(samples_matrix.T, samples_matrix, precision=lax.Precision.HIGHEST) / samples
    return 0.5 * (raw_gram + raw_gram.T) + jnp.diag(diagonal)


def draw_expert_grams(key, part):
    stacked = jnp.stack([one_gram(key, expert) for expert in range(EXPERTS)])
    return stacked.astype(jnp.float32)


def shard_levels(rng, shape, shards, least, high):
    factor_of = 1.0
    for axis_at, blocks in shards:
        steps = jax.random.uniform(jax.random.fold_in(jax.random.fold_in(rng, 6), axis_at), (blocks,), jnp.float32, least / len(shards), high / len(shards))
        factor_of = factor_of * jnp.repeat(jnp.exp(steps), shape[axis_at] // blocks).reshape((-1,) + (1,) * (len(shape) - 1 - axis_at))
    return factor_of


def bell_draw(own_key, extent, width, limit, cuts=(), kind=jnp.bfloat16):
    values = width * jax.random.normal(own_key, extent, jnp.float32)
    if cuts:
        values = values * shard_levels(own_key, extent, cuts, -0.22, 0.18)
    return jnp.clip(values, -limit, limit).astype(kind)


def setup_inputs(seed: int = 0) -> dict:
    seeds = jax.random.split(jax.random.key(seed), 3)
    expert_grams = draw_expert_grams(jax.random.fold_in(seeds[2], 71), 0)
    expert_weights = bell_draw(seeds[1], (EXPERTS, D, COLS), 1.0, 6.0, ((1, 8), (2, 4)))
    return dict(expert_grams=expert_grams, expert_weights=expert_weights)


def reference(expert_grams, expert_weights):
    system = lax.optimization_barrier(jnp.sum(expert_grams, axis=0)) + jnp.eye(D, dtype=jnp.float32)
    target = jnp.zeros((D, COLS), jnp.float32)
    for expert in range(EXPERTS):
        target = target + jnp.dot(expert_grams[expert], expert_weights[expert].astype(jnp.float32), precision=lax.Precision.HIGHEST, preferred_element_type=jnp.float32)
    merged = jnp.zeros((D, COLS), jnp.float32)
    residual = target
    direction = target
    norm_now = lax.optimization_barrier(jnp.sum(residual * residual, axis=0))
    initial = norm_now
    for iteration in range(ITERS):
        mapped = jnp.dot(system, direction, precision=lax.Precision.HIGHEST, preferred_element_type=jnp.float32)
        step_size = norm_now / lax.optimization_barrier(jnp.sum(direction * mapped, axis=0))
        merged = merged + step_size * direction
        residual = residual - step_size * mapped
        norm_next = lax.optimization_barrier(jnp.sum(residual * residual, axis=0))
        direction = residual + norm_next / norm_now * direction
        norm_now = norm_next
    residual_ratio = jnp.sqrt(jnp.sum(norm_now) / jnp.sum(initial))
    return (merged, residual_ratio)
```

```python
import functools

import jax
import jax.numpy as jnp
from jax import lax
from jax.experimental import pallas as pl
from jax.experimental.pallas import tpu as pltpu
from jax.sharding import PartitionSpec as P

ITERS = 4
SLOTS = 3
F32 = jnp.float32
BF16 = jnp.bfloat16


def split(x):
    high = x.astype(BF16)
    return high, (x - high.astype(F32)).astype(BF16)


def grid_side(chips):
    side = int(chips**0.5)
    while chips % side:
        side -= 1
    return chips // side


def kernel(
    n, groups,
    grams, weights, merged, ratio,
    panel, planes, wide, system, blocks, last_blocks,
    to_sibling, from_sibling, to_chip, from_chip,
    dots, totals, res, mapped, mapped_dir, second_dir, direction, second,
    gram_sem, sib_send, sib_recv, chip_send, chip_recv,
    block_send, block_recv, relay_send, dot_send, dot_recv, total_send, total_recv,
):
    experts, rows, columns = weights.shape
    chips = n // 2
    side = grid_side(chips)
    me = lax.axis_index("row")
    group = lax.axis_index("grp")
    core = lax.rem(me, 2)
    chip = me // 2
    sibling = chip * 2 + 1 - core

    def chip_at(t):
        up = lax.rem(chip // side + t // side, chips // side)
        return up * side + lax.rem(lax.rem(chip, side) + lax.rem(t, side), side)

    def chip_from(t):
        down = lax.rem(chip // side + chips // side - t // side, chips // side)
        return down * side + lax.rem(lax.rem(chip, side) + side - lax.rem(t, side), side)

    def chunk_of(c):
        t = chips - 1 - c // 2
        half = lax.rem(c, 2)
        owner = jnp.where(half == 0, 1 - core, core)
        return chip_at(t) * 2 + owner

    def gram_copy(c):
        start = pl.multiple_of(chunk_of(c) * rows, rows)
        slot = lax.rem(c, SLOTS)
        return pltpu.make_async_copy(
            grams.at[:, :, pl.ds(start, rows)], panel.at[slot], gram_sem.at[slot]
        )

    for c in range(SLOTS - 1):
        gram_copy(jnp.int32(c)).start()

    barrier = pltpu.get_barrier_semaphore()
    for other in range(1, n):
        pl.semaphore_signal(
            barrier, inc=1, device_id={"row": lax.rem(me + other, n)},
            device_id_type=pl.DeviceIdType.MESH,
        )
    for other in range(1, groups):
        pl.semaphore_signal(
            barrier, inc=1, device_id={"grp": lax.rem(group + other, groups)},
            device_id_type=pl.DeviceIdType.MESH,
        )

    for expert in range(experts):
        turned = weights[expert].astype(F32).T.astype(BF16)
        wide[:, expert * rows : (expert + 1) * rows] = turned
        wide[:, (experts + expert) * rows : (experts + expert + 1) * rows] = turned

    pl.semaphore_wait(barrier, n - 1 + groups - 1)

    def send(src, dst, send_sem, recv_sem, axis, index):
        return pltpu.make_async_remote_copy(
            src_ref=src, dst_ref=dst, send_sem=send_sem, recv_sem=recv_sem,
            device_id={axis: index}, device_id_type=pl.DeviceIdType.MESH,
        )

    def sibling_copy(t):
        return send(
            to_sibling.at[t], from_sibling.at[t], sib_send.at[t], sib_recv.at[t], "row", sibling
        )

    def chip_copy(t):
        return send(
            to_chip.at[t], from_chip.at[t], chip_send.at[t], chip_recv.at[t],
            "row", chip_at(t) * 2 + core,
        )

    def absorb(c):
        gram_copy(c).wait()

        @pl.when(c + SLOTS - 1 < n)
        def _():
            gram_copy(c + SLOTS - 1).start()

        slot = lax.rem(c, SLOTS)
        at = chunk_of(c)
        tile = min(64, rows)

        def fill(i, carry):
            top = pl.multiple_of(i * tile, tile)
            total = jnp.zeros((tile, rows), F32)
            for expert in range(experts):
                part = panel[slot, expert, pl.ds(top, tile), :]
                total = total + part
                high, low = split(part)
                planes[pl.ds(expert * rows + top, tile), :] = high
                planes[pl.ds((experts + expert) * rows + top, tile), :] = low
            row_ids = me * rows + top + lax.broadcasted_iota(jnp.int32, (tile, rows), 0)
            col_ids = at * rows + lax.broadcasted_iota(jnp.int32, (tile, rows), 1)
            total = total + jnp.where(row_ids == col_ids, 1.0, 0.0)
            high, low = split(total)
            system[at, pl.ds(top, tile), :] = high
            system[at, pl.ds(rows + top, tile), :] = low
            return carry

        lax.fori_loop(0, rows // tile, fill, 0)
        return jnp.dot(wide[...], planes[...], preferred_element_type=F32).T

    def pair(i, carry):
        t = chips - 1 - i
        to_sibling[t] = absorb(2 * i)
        sibling_copy(t).start()
        mine = absorb(2 * i + 1)
        sibling_copy(t).wait_recv()
        to_chip[t] = mine + from_sibling[t]

        @pl.when(t > 0)
        def _():
            chip_copy(t).start()

        return carry

    lax.fori_loop(0, chips, pair, 0)

    res[...] = to_chip[0]

    def collect(i, carry):
        t = chips - 1 - i
        chip_copy(t).wait_recv()
        res[...] += from_chip[t]
        return carry

    lax.fori_loop(0, chips - 1, collect, 0)

    def block_copy(k, t, source):
        return block_op(k, source, block_send.at[k, t], chip_at(t) * 2 + core)

    def block_op(k, source, send_sem, target):
        store = last_blocks if k == ITERS - 1 else blocks.at[k]
        return send(
            store.at[source], store.at[source], send_sem, block_recv.at[k, source], "row", target
        )

    def multiply(k, source):
        if k == ITERS - 1:
            second[...] += jnp.dot(
                system[source, :rows, :], last_blocks[source], preferred_element_type=F32
            )
        else:
            full = jnp.dot(system[source], blocks[k, source], preferred_element_type=F32)
            full = full[:rows] + full[rows:]
            second[...] += full[:, :columns] + full[:, columns:]

    def dot_copy(k, other):
        return send(
            dots.at[k, me], dots.at[k, me], dot_send.at[k, other], dot_recv.at[k, me],
            "row", lax.rem(me + other, n),
        )

    def dot_wait(k, other):
        source = lax.rem(me + other, n)
        return send(
            dots.at[k, source], dots.at[k, source], dot_send.at[k, other],
            dot_recv.at[k, source], "row", source,
        )

    def share(k, first, other=None):
        dots[k, me, 0:1, :] = first
        if other is not None:
            dots[k, me, 1:2, :] = other

        def go(o, carry):
            dot_copy(k, o).start()
            return carry

        lax.fori_loop(1, n, go, 0)

    def shared(k):
        def take(o, carry):
            dot_wait(k, o).wait_recv()
            return carry

        lax.fori_loop(1, n, take, 0)
        both = jnp.sum(dots[k], axis=0)
        return both[0:1, :], both[1:2, :]

    def column_sum(x):
        return jnp.sum(x, axis=0, keepdims=True)

    def spread(k, value):
        high, low = split(value)
        if k == ITERS - 1:
            last_blocks[me] = high
        else:
            blocks[k, me, :, :columns] = high
            blocks[k, me, :, columns:] = low
        block_op(k, me, relay_send.at[k, 0], sibling).start()

        def go(i, carry):
            block_copy(k, chips - 1 - i, me).start()
            return carry

        lax.fori_loop(0, chips - 1, go, 0)

    def product(k):
        second[...] = jnp.zeros_like(second)
        multiply(k, me)
        block_op(k, sibling, relay_send.at[k, 0], sibling).wait_recv()
        multiply(k, sibling)

        def take(t, carry):
            source = chip_from(t)
            near = source * 2 + core
            block_op(k, near, relay_send.at[k, t], sibling).wait_recv()
            block_op(k, near, relay_send.at[k, t], sibling).start()
            multiply(k, near)
            far = source * 2 + 1 - core
            block_op(k, far, relay_send.at[k, t], sibling).wait_recv()
            multiply(k, far)
            return carry

        lax.fori_loop(1, chips, take, 0)

    for k in range(ITERS + 1):
        dots[k, me] = jnp.zeros(dots.shape[2:], F32)

    spread(0, res[...])
    product(0)
    mapped[...] = second[...]
    mapped_dir[...] = jnp.zeros_like(mapped_dir)
    second_dir[...] = jnp.zeros_like(second_dir)
    direction[...] = jnp.zeros_like(direction)
    merged[...] = jnp.zeros_like(merged)

    initial = None
    norm_before = None
    step_before = None
    for k in range(ITERS):
        more = k + 1 < ITERS
        if more:
            spread(k + 1, mapped[...])
        share(k, column_sum(res[...] * res[...]), column_sum(res[...] * mapped[...]))
        if more:
            product(k + 1)
        norm, along = shared(k)
        if k == 0:
            initial = norm
            step = norm / along
            scaling = jnp.zeros_like(norm)
        else:
            scaling = norm / norm_before
            step = norm / (along - scaling * norm / step_before)
        norm_before, step_before = norm, step
        ahead = res[...] + scaling * direction[...]
        direction[...] = ahead
        merged[...] += step * ahead
        ahead = mapped[...] + scaling * mapped_dir[...]
        mapped_dir[...] = ahead
        res[...] -= step * ahead
        if more:
            ahead = second[...] + scaling * second_dir[...]
            second_dir[...] = ahead
            mapped[...] -= step * ahead

    share(ITERS, column_sum(res[...] * res[...]))
    final, _ = shared(ITERS)

    def total_copy(other):
        return send(
            totals.at[group], totals.at[group], total_send.at[other], total_recv.at[group],
            "grp", lax.rem(group + other, groups),
        )

    totals[group] = jnp.zeros(totals.shape[1:], F32)
    totals[group, 0:1, :] = final
    totals[group, 1:2, :] = initial
    for other in range(1, groups):
        total_copy(other).start()
    for other in range(1, groups):
        source = lax.rem(group + other, groups)
        send(
            totals.at[source], totals.at[source], total_send.at[other], total_recv.at[source],
            "grp", source,
        ).wait_recv()
    both = jnp.sum(jnp.sum(totals[...], axis=0), axis=1, keepdims=True)
    ratio[...] = jnp.broadcast_to(jnp.sqrt(both[0:1] / both[1:2]), ratio.shape)

    for other in range(1, groups):
        total_copy(other).wait_send()
    for k in range(ITERS + 1):
        def drain_dots(o, carry):
            dot_copy(k, o).wait_send()
            return carry

        lax.fori_loop(1, n, drain_dots, 0)
    for k in range(ITERS):
        block_op(k, me, relay_send.at[k, 0], sibling).wait_send()

        def drain_blocks(t, carry):
            block_copy(k, t, me).wait_send()
            block_op(k, me, relay_send.at[k, t], sibling).wait_send()
            return carry

        lax.fori_loop(1, chips, drain_blocks, 0)

    def drain_sums(t, carry):
        sibling_copy(t).wait_send()

        @pl.when(t > 0)
        def _():
            chip_copy(t).wait_send()

        return carry

    lax.fori_loop(0, chips, drain_sums, 0)


def local(n, groups, expert_grams, expert_weights):
    experts, rows, width = expert_grams.shape
    columns = expert_weights.shape[2]
    chips = n // 2
    vector = pltpu.VMEM((rows, columns), F32)
    dma = pltpu.SemaphoreType.DMA
    merged, ratio = pl.pallas_call(
        functools.partial(kernel, n, groups),
        out_shape=(
            jax.ShapeDtypeStruct((rows, columns), F32),
            jax.ShapeDtypeStruct((8, 128), F32),
        ),
        in_specs=[
            pl.BlockSpec(memory_space=pl.ANY),
            pl.BlockSpec(memory_space=pltpu.VMEM),
        ],
        out_specs=(
            pl.BlockSpec(memory_space=pltpu.VMEM),
            pl.BlockSpec(memory_space=pltpu.VMEM),
        ),
        scratch_shapes=[
            pltpu.VMEM((SLOTS, experts, rows, rows), F32),
            pltpu.VMEM((2 * experts * rows, rows), BF16),
            pltpu.VMEM((columns, 2 * experts * rows), BF16),
            pltpu.VMEM((n, 2 * rows, rows), BF16),
            pltpu.VMEM((ITERS - 1, n, rows, 2 * columns), BF16),
            pltpu.VMEM((n, rows, columns), BF16),
            pltpu.VMEM((chips, rows, columns), F32),
            pltpu.VMEM((chips, rows, columns), F32),
            pltpu.VMEM((chips, rows, columns), F32),
            pltpu.VMEM((chips, rows, columns), F32),
            pltpu.VMEM((ITERS + 1, n, 8, columns), F32),
            pltpu.VMEM((groups, 8, columns), F32),
            vector, vector, vector, vector, vector, vector,
            dma((SLOTS,)),
            dma((chips,)), dma((chips,)), dma((chips,)), dma((chips,)),
            dma((ITERS, chips)), dma((ITERS, n)), dma((ITERS, chips)),
            dma((ITERS + 1, n)), dma((ITERS + 1, n)), dma((groups,)), dma((groups,)),
        ],
        compiler_params=pltpu.CompilerParams(
            collective_id=0, has_side_effects=True, vmem_limit_bytes=60 * 1024 * 1024
        ),
    )(expert_grams, expert_weights)
    return merged, ratio[0, 0]


def solution(mesh):
    placed = (P(None, "row", None), P(None, "row", "grp"))
    body = functools.partial(local, mesh.shape["row"], mesh.shape["grp"])
    return jax.shard_map(
        body, mesh=mesh, in_specs=placed, out_specs=(P("row", "grp"), P()), check_vma=False
    )
```

```python
import functools

import jax
import jax.numpy as jnp
from jax import lax
from jax.experimental import pallas as pl
from jax.experimental.pallas import tpu as pltpu
from jax.sharding import PartitionSpec as P

ITERS = 4
SLOTS = 4
F32 = jnp.float32
BF16 = jnp.bfloat16


def split(x):
    high = x.astype(BF16)
    return high, (x - high.astype(F32)).astype(BF16)


def grid_side(chips):
    side = int(chips**0.5)
    while chips % side:
        side -= 1
    return chips // side


def kernel(
    n, groups,
    grams, weights, merged, ratio,
    panel, planes, wide, system, blocks, last_blocks,
    to_sibling, from_sibling, to_chip, from_chip,
    dots, totals, res, mapped, mapped_dir, second_dir, direction, second,
    gram_sem, sib_send, sib_recv, chip_send, chip_recv,
    block_send, block_recv, relay_send, hop_send, dot_send, dot_recv, total_send, total_recv,
):
    experts, rows, columns = weights.shape
    chips = n // 2
    side = grid_side(chips)
    me = lax.axis_index("row")
    group = lax.axis_index("grp")
    core = lax.rem(me, 2)
    chip = me // 2
    sibling = chip * 2 + 1 - core

    def chip_at(t):
        up = lax.rem(chip // side + t // side, chips // side)
        return up * side + lax.rem(lax.rem(chip, side) + lax.rem(t, side), side)

    def chip_from(t):
        down = lax.rem(chip // side + chips // side - t // side, chips // side)
        return down * side + lax.rem(lax.rem(chip, side) + side - lax.rem(t, side), side)

    def chunk_of(c):
        odd = lax.rem(c, 2) == 1
        t = jnp.where(odd, chips - 1 - (c + 1) // 2, chips - c // 2)
        t = jnp.where(c == 0, chips - 1, jnp.where(c == n - 1, 0, t))
        ahead = jnp.logical_or(c == 0, jnp.logical_and(odd, c < n - 1))
        return chip_at(t) * 2 + jnp.where(ahead, 1 - core, core)

    def gram_copy(c):
        start = pl.multiple_of(chunk_of(c) * rows, rows)
        slot = lax.rem(c, SLOTS)
        return pltpu.make_async_copy(
            grams.at[:, :, pl.ds(start, rows)], panel.at[slot], gram_sem.at[slot]
        )

    for c in range(SLOTS - 1):
        gram_copy(jnp.int32(c)).start()

    barrier = pltpu.get_barrier_semaphore()
    for other in range(1, n):
        pl.semaphore_signal(
            barrier, inc=1, device_id={"row": lax.rem(me + other, n)},
            device_id_type=pl.DeviceIdType.MESH,
        )
    for other in range(1, groups):
        pl.semaphore_signal(
            barrier, inc=1, device_id={"grp": lax.rem(group + other, groups)},
            device_id_type=pl.DeviceIdType.MESH,
        )

    for expert in range(experts):
        turned = weights[expert].astype(F32).T.astype(BF16)
        wide[:, expert * rows : (expert + 1) * rows] = turned
        wide[:, (experts + expert) * rows : (experts + expert + 1) * rows] = turned

    pl.semaphore_wait(barrier, n - 1 + groups - 1)

    def send(src, dst, send_sem, recv_sem, axis, index):
        return pltpu.make_async_remote_copy(
            src_ref=src, dst_ref=dst, send_sem=send_sem, recv_sem=recv_sem,
            device_id={axis: index}, device_id_type=pl.DeviceIdType.MESH,
        )

    def sibling_copy(t):
        return send(
            to_sibling.at[t], from_sibling.at[t], sib_send.at[t], sib_recv.at[t], "row", sibling
        )

    def chip_copy(t):
        return send(
            to_chip.at[t], from_chip.at[t], chip_send.at[t], chip_recv.at[t],
            "row", chip_at(t) * 2 + core,
        )

    def absorb(c):
        gram_copy(c).wait()

        @pl.when(c + SLOTS - 1 < n)
        def _():
            gram_copy(c + SLOTS - 1).start()

        slot = lax.rem(c, SLOTS)
        at = chunk_of(c)
        tile = min(64, rows)

        def fill(i, carry):
            top = pl.multiple_of(i * tile, tile)
            total = jnp.zeros((tile, rows), F32)
            for expert in range(experts):
                part = panel[slot, expert, pl.ds(top, tile), :]
                total = total + part
                high, low = split(part)
                planes[pl.ds(expert * rows + top, tile), :] = high
                planes[pl.ds((experts + expert) * rows + top, tile), :] = low
            row_ids = me * rows + top + lax.broadcasted_iota(jnp.int32, (tile, rows), 0)
            col_ids = at * rows + lax.broadcasted_iota(jnp.int32, (tile, rows), 1)
            total = total + jnp.where(row_ids == col_ids, 1.0, 0.0)
            high, low = split(total)
            system[at, pl.ds(top, tile), :] = high
            system[at, pl.ds(rows + top, tile), :] = low
            return carry

        lax.fori_loop(0, rows // tile, fill, 0)
        return jnp.dot(wide[...], planes[...], preferred_element_type=F32).T

    def hand_over(c, t):
        to_sibling[t] = absorb(c)
        sibling_copy(t).start()

    def combine(c, t):
        mine = absorb(c)
        sibling_copy(t).wait_recv()
        return mine + from_sibling[t]

    hand_over(jnp.int32(0), chips - 1)

    def pair(i, carry):
        hand_over(2 * i + 1, chips - 2 - i)
        t = chips - 1 - i
        to_chip[t] = combine(2 * i + 2, t)
        chip_copy(t).start()
        return carry

    lax.fori_loop(0, chips - 1, pair, 0)

    res[...] = combine(jnp.int32(n - 1), 0)

    def collect(i, carry):
        t = chips - 1 - i
        chip_copy(t).wait_recv()
        res[...] += from_chip[t]
        return carry

    lax.fori_loop(0, chips - 1, collect, 0)

    half = rows // 2
    relayed = chips == 4 and side == 2

    def block_op(k, source, h, send_sem, target):
        store = last_blocks if k == ITERS - 1 else blocks.at[k]
        piece = store.at[source, h * half : (h + 1) * half]
        return send(piece, piece, send_sem, block_recv.at[k, source, h], "row", target)

    def to_far(k, t, h):
        return block_op(k, me, h, block_send.at[k, t, h], chip_at(t) * 2 + core)

    def to_near(k, t, h, source):
        return block_op(k, source, h, relay_send.at[k, t, h], sibling)

    def multiply(k, source):
        if k == ITERS - 1:
            second[...] += jnp.dot(
                system[source, :rows, :], last_blocks[source], preferred_element_type=F32
            )
        else:
            full = jnp.dot(system[source], blocks[k, source], preferred_element_type=F32)
            full = full[:rows] + full[rows:]
            second[...] += full[:, :columns] + full[:, columns:]

    def dot_copy(k, other):
        return send(
            dots.at[k, me], dots.at[k, me], dot_send.at[k, other], dot_recv.at[k, me],
            "row", lax.rem(me + other, n),
        )

    def dot_wait(k, other):
        source = lax.rem(me + other, n)
        return send(
            dots.at[k, source], dots.at[k, source], dot_send.at[k, other],
            dot_recv.at[k, source], "row", source,
        )

    def share(k, first, other=None):
        dots[k, me, 0:1, :] = first
        if other is not None:
            dots[k, me, 1:2, :] = other

        def go(o, carry):
            dot_copy(k, o).start()
            return carry

        lax.fori_loop(1, n, go, 0)

    def shared(k):
        def take(o, carry):
            dot_wait(k, o).wait_recv()
            return carry

        lax.fori_loop(1, n, take, 0)
        sums = jnp.sum(dots[k], axis=0)
        return sums[0:1, :], sums[1:2, :]

    def column_sum(x):
        return jnp.sum(x, axis=0, keepdims=True)

    def spread(k, value):
        high, low = split(value)
        if k == ITERS - 1:
            last_blocks[me] = high
        else:
            blocks[k, me, :, :columns] = high
            blocks[k, me, :, columns:] = low
        if relayed:
            for t, h in ((1, 0), (2, 1)):
                to_far(k, t, h).start()
            for h in (0, 1):
                to_near(k, 0, h, me).start()
            for t, h in ((1, 1), (2, 0)):
                to_far(k, t, h).start()
            return
        for h in (0, 1):
            to_near(k, 0, h, me).start()

        def go(i, carry):
            for h in (0, 1):
                to_far(k, chips - 1 - i, h).start()
            return carry

        lax.fori_loop(0, chips - 1, go, 0)

    def both(k, first, other):
        def one(i, carry):
            multiply(k, jnp.where(i == 0, first, other))
            return carry

        lax.fori_loop(0, 2, one, 0)

    def arrive(k, source, h):
        to_near(k, 0, h, source).wait_recv()

    def hop(k, h, source):
        return block_op(k, source, h, hop_send.at[k, h], chip_at(2 - h) * 2 + core)

    def product(k):
        second[...] = jnp.zeros_like(second)
        for h in (0, 1):
            arrive(k, sibling, h)
        both(k, me, sibling)
        if relayed:
            by_x, by_y, by_both = (chip_at(t) * 2 for t in (1, 2, 3))
            for t, h, source in ((1, 0, by_x), (2, 1, by_y)):
                arrive(k, source + core, h)
                hop(k, h, source + core).start()
                to_near(k, t, h, source + core).start()
            for t, h, source in ((1, 1, by_x), (2, 0, by_y)):
                arrive(k, source + core, h)
                to_near(k, t, h, source + core).start()
            both(k, by_x + core, by_y + core)
            for source in (by_x, by_y):
                for h in (0, 1):
                    arrive(k, source + 1 - core, h)
            both(k, by_x + 1 - core, by_y + 1 - core)
            for h in (0, 1):
                arrive(k, by_both + core, h)
                to_near(k, 3, h, by_both + core).start()
            multiply(k, by_both + core)
            for h in (0, 1):
                arrive(k, by_both + 1 - core, h)
            multiply(k, by_both + 1 - core)
            return

        def take(i, carry):
            t = chips - 1 - i
            near = chip_from(t) * 2 + core
            for h in (0, 1):
                arrive(k, near, h)
                to_near(k, t, h, near).start()
            multiply(k, near)
            far = chip_from(t) * 2 + 1 - core
            for h in (0, 1):
                arrive(k, far, h)
            multiply(k, far)
            return carry

        lax.fori_loop(0, chips - 1, take, 0)

    for k in range(ITERS + 1):
        dots[k, me] = jnp.zeros(dots.shape[2:], F32)

    spread(0, res[...])
    product(0)
    mapped[...] = second[...]
    mapped_dir[...] = jnp.zeros_like(mapped_dir)
    second_dir[...] = jnp.zeros_like(second_dir)
    direction[...] = jnp.zeros_like(direction)
    merged[...] = jnp.zeros_like(merged)

    initial = None
    norm_before = None
    step_before = None
    for k in range(ITERS):
        more = k + 1 < ITERS
        if more:
            spread(k + 1, mapped[...])
        share(k, column_sum(res[...] * res[...]), column_sum(res[...] * mapped[...]))
        if more:
            product(k + 1)
        norm, along = shared(k)
        if k == 0:
            initial = norm
            step = norm / along
            scaling = jnp.zeros_like(norm)
        else:
            scaling = norm / norm_before
            step = norm / (along - scaling * norm / step_before)
        norm_before, step_before = norm, step
        ahead = res[...] + scaling * direction[...]
        direction[...] = ahead
        merged[...] += step * ahead
        ahead = mapped[...] + scaling * mapped_dir[...]
        mapped_dir[...] = ahead
        res[...] -= step * ahead
        if more:
            ahead = second[...] + scaling * second_dir[...]
            second_dir[...] = ahead
            mapped[...] -= step * ahead

    share(ITERS, column_sum(res[...] * res[...]))
    final, _ = shared(ITERS)

    def total_copy(other):
        return send(
            totals.at[group], totals.at[group], total_send.at[other], total_recv.at[group],
            "grp", lax.rem(group + other, groups),
        )

    totals[group] = jnp.zeros(totals.shape[1:], F32)
    totals[group, 0:1, :] = final
    totals[group, 1:2, :] = initial
    for other in range(1, groups):
        total_copy(other).start()
    for other in range(1, groups):
        source = lax.rem(group + other, groups)
        send(
            totals.at[source], totals.at[source], total_send.at[other], total_recv.at[source],
            "grp", source,
        ).wait_recv()
    sums = jnp.sum(jnp.sum(totals[...], axis=0), axis=1, keepdims=True)
    ratio[...] = jnp.broadcast_to(jnp.sqrt(sums[0:1] / sums[1:2]), ratio.shape)

    for other in range(1, groups):
        total_copy(other).wait_send()
    for k in range(ITERS + 1):
        def drain_dots(o, carry):
            dot_copy(k, o).wait_send()
            return carry

        lax.fori_loop(1, n, drain_dots, 0)
    for k in range(ITERS):
        for h in (0, 1):
            to_near(k, 0, h, me).wait_send()
            if relayed:
                hop(k, h, me).wait_send()

        def drain_near(t, carry):
            for h in (0, 1):
                to_near(k, t, h, me).wait_send()
            return carry

        lax.fori_loop(1, chips, drain_near, 0)

        def drain_far(t, carry):
            for h in (0, 1):
                to_far(k, t, h).wait_send()
            return carry

        lax.fori_loop(1, chips - 1 if relayed else chips, drain_far, 0)

    def drain_sums(t, carry):
        sibling_copy(t).wait_send()

        @pl.when(t > 0)
        def _():
            chip_copy(t).wait_send()

        return carry

    lax.fori_loop(0, chips, drain_sums, 0)


def local(n, groups, expert_grams, expert_weights):
    experts, rows, width = expert_grams.shape
    columns = expert_weights.shape[2]
    chips = n // 2
    vector = pltpu.VMEM((rows, columns), F32)
    dma = pltpu.SemaphoreType.DMA
    merged, ratio = pl.pallas_call(
        functools.partial(kernel, n, groups),
        out_shape=(
            jax.ShapeDtypeStruct((rows, columns), F32),
            jax.ShapeDtypeStruct((8, 128), F32),
        ),
        in_specs=[
            pl.BlockSpec(memory_space=pl.ANY),
            pl.BlockSpec(memory_space=pltpu.VMEM),
        ],
        out_specs=(
            pl.BlockSpec(memory_space=pltpu.VMEM),
            pl.BlockSpec(memory_space=pltpu.VMEM),
        ),
        scratch_shapes=[
            pltpu.VMEM((SLOTS, experts, rows, rows), F32),
            pltpu.VMEM((2 * experts * rows, rows), BF16),
            pltpu.VMEM((columns, 2 * experts * rows), BF16),
            pltpu.VMEM((n, 2 * rows, rows), BF16),
            pltpu.VMEM((ITERS - 1, n, rows, 2 * columns), BF16),
            pltpu.VMEM((n, rows, columns), BF16),
            pltpu.VMEM((chips, rows, columns), F32),
            pltpu.VMEM((chips, rows, columns), F32),
            pltpu.VMEM((chips, rows, columns), F32),
            pltpu.VMEM((chips, rows, columns), F32),
            pltpu.VMEM((ITERS + 1, n, 8, columns), F32),
            pltpu.VMEM((groups, 8, columns), F32),
            vector, vector, vector, vector, vector, vector,
            dma((SLOTS,)),
            dma((chips,)), dma((chips,)), dma((chips,)), dma((chips,)),
            dma((ITERS, chips, 2)), dma((ITERS, n, 2)), dma((ITERS, chips, 2)), dma((ITERS, 2)),
            dma((ITERS + 1, n)), dma((ITERS + 1, n)), dma((groups,)), dma((groups,)),
        ],
        compiler_params=pltpu.CompilerParams(
            collective_id=0, has_side_effects=True, vmem_limit_bytes=60 * 1024 * 1024
        ),
    )(expert_grams, expert_weights)
    return merged, ratio[0, 0]


def solution(mesh):
    placed = (P(None, "row", None), P(None, "row", "grp"))
    body = functools.partial(local, mesh.shape["row"], mesh.shape["grp"])
    return jax.shard_map(
        body, mesh=mesh, in_specs=placed, out_specs=(P("row", "grp"), P()), check_vma=False
    )
```
